256 devices in a mesh: dp: 64 (over z, y, core), tensor: 4 (over x).
Axes of the slice: x: 4, y: 4, z: 8, core: 2. Of those that a mesh axis runs over, the one named last changes fastest.
Arguments:
- tokens: bfloat16 [131072, 4096], P('dp', 'tensor'), may hold values from -16 to 16
- cotangent: bfloat16 [131072, 1536], P('dp', 'tensor'), may hold values from -0.059814453 to 0.059814453
- seg_start: int32 [64, 2], P('dp'), may hold values from 0 to 1024, as said below
- seg_length: int32 [64, 2], P('dp'), may hold values from 0 to 1024, as said below
Outputs:
- weight_grad: float32 [4096, 2, 1536], P('dp', None, 'tensor')
The draws below stay inside these ranges and needn't reach their ends.
Inputs may be any that keep to these rules, and one draw needn't show every extreme that they name: Within each index of dp the 2 segments lie in expert order, packed from row 0 without gaps: seg_start is the running sum of seg_length before each expert. `seg_length`: each length is at most 1024; in every draw some expert on some index of dp has exactly 1024 rows. Rows after the last segment belong to no expert.
All inputs are finite; a program needn't handle non-finite values.
Results may differ from the reference program's by a relative error of at most 0.0003.
Values may be sent and summed in bfloat16 or wider, within the bound.
A program may use at most 128 MiB of HBM per device.

```python
import jax
import jax.numpy as jnp
from jax import lax

D = 4096
FF = 1536
E_W = 2
CAP = 1024
TOKENS = 131072
N_DP = 64


def segment_bounds(key):
    keys = jax.random.split(jax.random.fold_in(key, 7), 4)
    load = jax.random.randint(keys[0], (N_DP, 1), 1, 5)
    lower = load * CAP // 8
    upper = load * CAP // 4 + 1
    draws = jax.random.randint(keys[1], (N_DP, E_W), 0, 1 << 30)
    length = lower + draws % (upper - lower)
    busy_device = jax.random.randint(keys[2], (), 0, N_DP)
    busy_expert = jax.random.randint(keys[3], (), 0, E_W)
    hit = (jnp.arange(N_DP)[:, None] == busy_device) & (jnp.arange(E_W)[None, :] == busy_expert)
    length = jnp.where(hit, CAP, length)
    start = jnp.cumsum(length, axis=1) - length
    return (start.astype(jnp.int32), length.astype(jnp.int32))


def draw_seg_start(key, part):
    return segment_bounds(key)[0]


def draw_seg_length(key, part):
    return segment_bounds(key)[1]


def with_spikes(values, rng, source, target, shards_of, factor):
    owner, partner = [(jnp.arange(values.shape[axis_at]) // (values.shape[axis_at] // shards_of)).reshape([-1 if axis == axis_at else 1 for axis in range(values.ndim)]) for axis_at in (source, target)]
    chosen = jax.random.permutation(rng, shards_of)[partner]
    strong = (owner == chosen) | (owner == (partner + shards_of // 2) % shards_of)
    return jnp.where(strong, factor * values, values)


def level_of(own_key, extent, shards, low, high):
    factor_of = 1.0
    for position, parts in shards:
        steps = jax.random.uniform(jax.random.fold_in(jax.random.fold_in(own_key, 6), position), (parts,), jnp.float32, low / len(shards), high / len(shards))
        factor_of = factor_of * jnp.repeat(jnp.exp(steps), extent[position] // parts).reshape((-1,) + (1,) * (len(extent) - 1 - position))
    return factor_of


def noise(key, extent, scale, bound, cuts=(), kind=jnp.bfloat16):
    values = jax.random.normal(key, extent, jnp.float32) * scale
    if len(cuts) > 0:
        values = level_of(key, extent, cuts, -0.22, 0.18) * values
    return jnp.clip(values, min=-bound, max=bound).astype(kind)


def bell_draw_with(stream_key, shape, width, bound, cuts, heavy, kind=jnp.bfloat16):
    drawn = width * jax.random.normal(stream_key, shape, jnp.float32)
    if cuts:
        drawn = drawn * level_of(stream_key, shape, cuts, -0.22, 0.18)
    return jnp.clip(with_spikes(drawn, jax.random.fold_in(stream_key, 3), *heavy), -bound, bound).astype(kind)


def setup_inputs(seed: int = 0) -> dict:
    splits = jax.random.split(jax.random.key(seed), 5)
    tokens = bell_draw_with(splits[0], (TOKENS, D), 1.0, 16.0, ((0, 64), (1, 4)), (0, 1, 64, 4.0))
    cotangent = noise(splits[1], (TOKENS, FF), 0.01, 0.059814453, ((0, 64), (1, 4)))
    seg_start = draw_seg_start(jax.random.fold_in(splits[4], 71), 0)
    seg_length = draw_seg_length(jax.random.fold_in(splits[4], 71), 0)
    return dict(tokens=tokens, cotangent=cotangent, seg_start=seg_start, seg_length=seg_length)


def reference(tokens, cotangent, seg_start, seg_length):
    tok = E_W * CAP

    def peer(total, index):
        rows_x = lax.dynamic_slice_in_dim(tokens, index * tok, tok, 0)
        rows_g = lax.dynamic_slice_in_dim(cotangent, index * tok, tok, 0)
        terms = []
        for expert in range(E_W):
            start = seg_start[index, expert].astype(jnp.int32)
            length = seg_length[index, expert].astype(jnp.int32)
            first = jnp.minimum(start, tok - CAP).astype(jnp.int32)
            rows = first + jnp.arange(CAP, dtype=jnp.int32)
            keep = (rows >= start) & (rows < start + length)
            block_x = lax.dynamic_slice_in_dim(rows_x, first, CAP, 0)
            block_g = lax.dynamic_slice_in_dim(rows_g, first, CAP, 0)
            block_g = jnp.where(keep[:, None], block_g, jnp.zeros_like(block_g))
            terms.append(jnp.dot(block_x.T, block_g, preferred_element_type=jnp.float32))
        return total + jnp.stack(terms, 1), None

    start_total = jnp.zeros((D, E_W, FF), jnp.float32)
    total, unused = lax.scan(peer, start_total, jnp.arange(N_DP, dtype=jnp.int32))
    return total
```

```python
import jax
import jax.numpy as jnp
from jax import lax
from jax.experimental import pallas as pl
from jax.experimental.pallas import tpu as pltpu
from jax.sharding import PartitionSpec as P

MESH = pl.DeviceIdType.MESH
CAP = 1024
FEATS = 1024
L = 128
SUBS = 3
OWN, LEFT, RIGHT, OPP = 0, 1, 2, 3
X_OFF = {OWN: 0, LEFT: 3, RIGHT: 1, OPP: 2}
ORDER = (
    [(OWN, s) for s in range(SUBS)]
    + [(side, s) for s in range(SUBS) for side in (LEFT, RIGHT)]
    + [(OPP, s) for s in range(SUBS)]
)
N_Q = len(ORDER)
Q_OF = {slot_s: q for q, slot_s in enumerate(ORDER)}
BLOCKS = FEATS // L


def kernel(
    tok_hbm, cot_hbm, start_ref, length_ref, out_ref,
    xin, gin, xt, xsend, gbuf, gsend, p, y1, y2, zb, fin, ob,
    in_sem, gd_s, gd_r, xd_s, xd_r, gx_s, gx_r, y1_s, y1_r, y2_s, y2_r, z_s, z_r, f_s, f_r,
):
    t = lax.axis_index("tensor")
    dp = lax.axis_index("dp")
    z, y, e = dp // 8, (dp // 2) % 4, dp % 2

    def dev(x, y, z, c):
        return (z * 8 + y * 2 + c, x)

    def remote(src, dst, s, r, to):
        return pltpu.make_async_remote_copy(
            src_ref=src, dst_ref=dst, send_sem=s, recv_sem=r, device_id=to, device_id_type=MESH
        )

    def wait(ref, sem):
        pltpu.make_async_copy(ref, ref, sem).wait()

    partner = dev(t, y, z, 1 - e)
    right, left = dev((t + 1) % 4, y, z, e), dev((t + 3) % 4, y, z, e)
    y_a, y_b = y + 1 - 2 * (y % 2), 3 - y
    dev_a, dev_b = dev(t, y_a, z, e), dev(t, y_b, z, e)
    dest_z, dest_c = 2 * t + z // 4, (z // 2) % 2
    own_dest = (dest_z == z) & (dest_c == e)

    g_load = pltpu.make_async_copy(cot_hbm, gin, in_sem.at[0])
    x_load = pltpu.make_async_copy(tok_hbm, xin, in_sem.at[1])
    g_load.start()
    x_load.start()

    barrier = pltpu.get_barrier_semaphore()

    def greet(to):
        pl.semaphore_signal(barrier, inc=1, device_id=to, device_id_type=MESH)

    for to in (partner, right, left, dev_a, dev_b):
        greet(to)
    for d in range(1, 8):
        greet(dev(t, y, (z + d) % 8, e))
    for half in range(2):
        for c in range(2):
            sx, sz = z // 2, 4 * (z % 2) + 2 * e + half

            @pl.when(jnp.logical_not((sx == t) & (sz == z) & (c == e)))
            def _():
                greet(dev(sx, y, sz, c))

    def bounds(expert):
        first = start_ref[0, expert]
        return first, first + length_ref[0, expert]

    def pick(low, high, row, first):
        return jnp.where(row >= first, low, high)

    row = lax.broadcasted_iota(jnp.int32, (CAP, L), 0)
    (f0, l0), (f1, l1) = bounds(0), bounds(1)
    first_me, last_me = f0 + e * (f1 - f0), l0 + e * (l1 - l0)
    first_it, last_it = f1 + e * (f0 - f1), l1 + e * (l0 - l1)

    def cot_of(s, first, last):
        low = gin[:CAP, s * L : (s + 1) * L].astype(jnp.float32)
        high = gin[CAP:, s * L : (s + 1) * L].astype(jnp.float32)
        source_row = row + jnp.where(row >= first, 0, CAP)
        value = jnp.where(source_row < last, pick(low, high, row, first), 0.0)
        return value.astype(jnp.bfloat16)

    g_load.wait()
    for s in range(SUBS):
        gsend[s] = cot_of(s, first_it, last_it)
        gbuf[s, e] = cot_of(s, first_me, last_me)
    pl.semaphore_wait(barrier, 16 - jnp.where(own_dest, 1, 0))

    def give(s, src):
        unit = gbuf.at[s, src]
        q = Q_OF[LEFT, s]
        remote(unit, gbuf.at[q, src], gx_s.at[s, 0, src], gx_r.at[q - SUBS, src], right).start()
        q = Q_OF[RIGHT, s]
        remote(unit, gbuf.at[q, src], gx_s.at[s, 1, src], gx_r.at[q - SUBS, src], left).start()

    for s in range(SUBS):
        remote(gsend.at[s], gbuf.at[s, e], gd_s.at[s], gd_r.at[s], partner).start()
    give(0, e)
    for s in range(SUBS):
        wait(gbuf.at[s, 1 - e], gd_r.at[s])
        give(s, 1 - e)
        if s + 1 < SUBS:
            give(s + 1, e)

    x_load.wait()
    for fb in range(BLOCKS):
        cols = slice(fb * L, (fb + 1) * L)
        low = xin[:CAP, cols].astype(jnp.float32)
        high = xin[CAP:, cols].astype(jnp.float32)
        xsend[cols, :] = pick(low, high, row, first_it).T.astype(jnp.bfloat16)
        remote(xsend.at[cols, :], xt.at[e, cols, :], xd_s, xd_r, partner).start()
        xt[e, cols, :] = pick(low, high, row, first_me).T.astype(jnp.bfloat16)
    wait(xt.at[1 - e], xd_r)

    def multiply(q):
        slot, s = ORDER[q]
        if slot != OWN:
            for src in range(2):
                wait(gbuf.at[q, src], gx_r.at[q - SUBS, src])
        o = Q_OF[OPP, s]
        if slot == LEFT:
            remote(gbuf.at[q, 0], gbuf.at[o, 0], gx_s.at[s, 2, 0], gx_r.at[o - SUBS, 0], right).start()
        if slot == RIGHT:
            remote(gbuf.at[q, 1], gbuf.at[o, 1], gx_s.at[s, 2, 1], gx_r.at[o - SUBS, 1], left).start()

        def block(m, carry):
            rows = pl.ds(pl.multiple_of(m * L, L), L)
            p[q, m] = jnp.dot(
                xt[0, rows, :], gbuf[q, 0], preferred_element_type=jnp.float32
            ) + jnp.dot(xt[1, rows, :], gbuf[q, 1], preferred_element_type=jnp.float32)
            return carry

        lax.fori_loop(0, BLOCKS, block, 0)
        remote(p.at[q, 3 - y_a], y1.at[q, 0, 1], y1_s.at[q], y1_r.at[q], dev_a).start()
        remote(p.at[q, 4 + y_b + 1 - 2 * (y_b % 2)], y1.at[q, 1, 1], y1_s.at[q], y1_r.at[q], dev_b).start()
        remote(p.at[q, y_a], y1.at[q, 0, 0], y1_s.at[q], y1_r.at[q], dev_a).start()
        remote(p.at[q, 4 + y_b], y1.at[q, 1, 0], y1_s.at[q], y1_r.at[q], dev_b).start()

    def second(q):
        wait(y1.at[q], y1_r.at[q])
        p[q, y_b] += y1[q, 0, 1]
        remote(p.at[q, y_b], y2.at[q, 0], y2_s.at[q], y2_r.at[q], dev_b).start()
        p[q, 4 + y_a] += y1[q, 1, 1]
        remote(p.at[q, 4 + y_a], y2.at[q, 1], y2_s.at[q], y2_r.at[q], dev_a).start()
        p[q, y] += y1[q, 0, 0]
        p[q, 4 + y] += y1[q, 1, 0]

    def piece(q, zz):
        return p.at[q, (zz // 4) * 4 + y, pl.ds(pl.multiple_of((zz % 4) * 32, 32), 32), :]

    def third(q):
        wait(y2.at[q], y2_r.at[q])
        p[q, y] += y2[q, 0]
        p[q, 4 + y] += y2[q, 1]
        for d in (4, 3, 5, 2, 6, 1, 7):
            zz = (z + d) % 8
            remote(piece(q, zz), zb.at[q, d - 1], z_s.at[q], z_r.at[q], dev(t, y, zz, e)).start()

    def last(q):
        slot, s = ORDER[q]
        wait(zb.at[q], z_r.at[q])
        total = piece(q, z)[...]
        for d in range(7):
            total += zb[q, d]
        fin[q] = total
        to = dev((t + X_OFF[slot]) % 4, y, dest_z, dest_c)
        place = ob.at[e, s, z % 2]
        if slot == OWN:

            @pl.when(own_dest)
            def _():
                pltpu.make_async_copy(fin.at[q], place, f_r).start()

            @pl.when(jnp.logical_not(own_dest))
            def _():
                remote(fin.at[q], place, f_s.at[q], f_r, to).start()
        else:
            remote(fin.at[q], place, f_s.at[q], f_r, to).start()

    for step in range(N_Q + 3):
        if step < N_Q:
            multiply(step)
        if 0 <= step - 1 < N_Q:
            second(step - 1)
        if 0 <= step - 2 < N_Q:
            third(step - 2)
        if 0 <= step - 3 < N_Q:
            last(step - 3)

    wait(ob, f_r)
    for c in range(2):
        for s in range(SUBS):
            for half in range(2):
                out_ref[c, half * 32 : (half + 1) * 32, s * L : (s + 1) * L] = ob[c, s, half]

    for s in range(SUBS):
        wait(gsend.at[s], gd_s.at[s])
        for way in range(3):
            for src in range(2):
                wait(gbuf.at[s, src], gx_s.at[s, way, src])
    wait(xsend, xd_s)
    for q in range(N_Q):
        wait(y1.at[q], y1_s.at[q])
        wait(y2.at[q], y2_s.at[q])
        wait(zb.at[q], z_s.at[q])
        if ORDER[q][0] == OWN:

            @pl.when(jnp.logical_not(own_dest))
            def _():
                wait(fin.at[q], f_s.at[q])
        else:
            wait(fin.at[q], f_s.at[q])


def per_device(tokens, cotangent, seg_start, seg_length):
    dma = pltpu.SemaphoreType.DMA
    bf16, f32 = jnp.bfloat16, jnp.float32
    out = pl.pallas_call(
        kernel,
        out_shape=jax.ShapeDtypeStruct((2, 64, SUBS * L), f32),
        in_specs=[pl.BlockSpec(memory_space=pl.ANY)] * 2 + [pl.BlockSpec(memory_space=pltpu.SMEM)] * 2,
        out_specs=pl.BlockSpec(memory_space=pltpu.VMEM),
        scratch_shapes=[
            pltpu.VMEM((2 * CAP, FEATS), bf16),
            pltpu.VMEM((2 * CAP, SUBS * L), bf16),
            pltpu.VMEM((2, FEATS, CAP), bf16),
            pltpu.VMEM((FEATS, CAP), bf16),
            pltpu.VMEM((N_Q, 2, CAP, L), bf16),
            pltpu.VMEM((SUBS, CAP, L), bf16),
            pltpu.VMEM((N_Q, BLOCKS, L, L), f32),
            pltpu.VMEM((N_Q, 2, 2, L, L), f32),
            pltpu.VMEM((N_Q, 2, L, L), f32),
            pltpu.VMEM((N_Q, 7, 32, L), f32),
            pltpu.VMEM((N_Q, 32, L), f32),
            pltpu.VMEM((2, SUBS, 2, 32, L), f32),
            dma((2,)),
            dma((SUBS,)), dma((SUBS,)), dma, dma,
            dma((SUBS, 3, 2)), dma((N_Q - SUBS, 2)),
            dma((N_Q,)), dma((N_Q,)), dma((N_Q,)), dma((N_Q,)), dma((N_Q,)), dma((N_Q,)),
            dma((N_Q,)), dma,
        ],
        compiler_params=pltpu.CompilerParams(
            collective_id=0, has_side_effects=True, vmem_limit_bytes=60 * 1024 * 1024
        ),
        cost_estimate=pl.CostEstimate(flops=6442450944, bytes_accessed=6000000, transcendentals=0),
    )(tokens, cotangent, seg_start, seg_length)
    return out.transpose(1, 0, 2)


def solution(mesh):
    in_specs = (P("dp", "tensor"), P("dp", "tensor"), P("dp", None), P("dp", None))
    out_specs = P("dp", None, "tensor")
    return jax.shard_map(
        per_device, mesh=mesh, in_specs=in_specs, out_specs=out_specs, check_vma=False
    )
```

```python
import jax
import jax.numpy as jnp
from jax import lax
from jax.experimental import pallas as pl
from jax.experimental.pallas import tpu as pltpu
from jax.sharding import PartitionSpec as P

MESH = pl.DeviceIdType.MESH
CAP = 1024
FEATS = 1024
L = 128
SUBS = 3
OWN, LEFT, RIGHT, OPP = 0, 1, 2, 3
X_OFF = {OWN: 0, LEFT: 3, RIGHT: 1, OPP: 2}
ORDER = (
    [(OWN, s) for s in range(SUBS)]
    + [(side, s) for s in range(SUBS) for side in (LEFT, RIGHT)]
    + [(OPP, s) for s in range(SUBS)]
)
N_Q = len(ORDER)
Q_OF = {slot_s: q for q, slot_s in enumerate(ORDER)}
BLOCKS = FEATS // L
SPLIT = (N_Q - 1,)
PLAN = (
    "m0,1", "a1", "a0", "m2", "a2", "b1", "m3,4", "a4", "a3", "b0", "b2", "c1", "b4", "m5,6", "a5", "a6",
    "b3", "c0", "d1", "c2", "c4", "b5", "d0", "b6", "m7,8", "a8", "a7", "c3", "d2", "c5", "c6", "d4", "m9",
    "a9", "b8", "d3", "b7", "m10", "a10", "b9", "d5", "c8", "d6", "c7", "m11", "c9", "b10", "d8", "b11",
    "B11", "c10", "d7", "c11", "C11", "d9", "d10", "d11",
)
HALF = FEATS // 2


def kernel(
    tok_hbm, cot_hbm, start_ref, length_ref, out_ref,
    xin, gin, xt, xsend, gbuf, gsend, p, y1, y2, zb, fin, ob,
    in_sem, gd_s, gd_r, xd_s, xd_r, gx_s, gx_r, y1_s, y1_r, y2_s, y2_r, z_s, z_r, f_s, f_r,
):
    t = lax.axis_index("tensor")
    dp = lax.axis_index("dp")
    z, y, e = dp // 8, (dp // 2) % 4, dp % 2

    def dev(x, y, z, c):
        return (z * 8 + y * 2 + c, x)

    def remote(src, dst, s, r, to):
        return pltpu.make_async_remote_copy(
            src_ref=src, dst_ref=dst, send_sem=s, recv_sem=r, device_id=to, device_id_type=MESH
        )

    def wait(ref, sem):
        pltpu.make_async_copy(ref, ref, sem).wait()

    partner = dev(t, y, z, 1 - e)
    right, left = dev((t + 1) % 4, y, z, e), dev((t + 3) % 4, y, z, e)
    y_a, y_b = y + 1 - 2 * (y % 2), 3 - y
    dev_a, dev_b = dev(t, y_a, z, e), dev(t, y_b, z, e)

    def rank(zz):
        return (zz - 2 * t + 11) % 8

    my_rank = rank(z)
    dest_z, dest_c = 2 * t + my_rank // 4, (my_rank // 2) % 2
    own_dest = (dest_z == z) & (dest_c == e)

    g_loads = [
        pltpu.make_async_copy(cot_hbm.at[:, cols], gin.at[:, cols], in_sem.at[s])
        for s, cols in enumerate(pl.ds(s * L, L) for s in range(SUBS))
    ]
    x_loads = [
        pltpu.make_async_copy(tok_hbm.at[:, cols], xin.at[:, cols], in_sem.at[SUBS + i])
        for i, cols in enumerate(pl.ds(i * 2 * L, 2 * L) for i in range(BLOCKS // 2))
    ]
    for load in g_loads:
        load.start()

    barrier = pltpu.get_barrier_semaphore()

    def greet(to):
        pl.semaphore_signal(barrier, inc=1, device_id=to, device_id_type=MESH)

    for to in (partner, right, left, dev_a, dev_b):
        greet(to)
    for d in range(1, 8):
        greet(dev(t, y, (z + d) % 8, e))
    for half in range(2):
        for c in range(2):
            sx = z // 2
            sz = (4 * (z % 2) + 2 * e + half + 2 * sx + 5) % 8

            @pl.when(jnp.logical_not((sx == t) & (sz == z) & (c == e)))
            def _():
                greet(dev(sx, y, sz, c))

    def bounds(expert):
        first = start_ref[0, expert]
        return first, first + length_ref[0, expert]

    def pick(low, high, row, first):
        return jnp.where(row >= first, low, high)

    row = lax.broadcasted_iota(jnp.int32, (CAP, L), 0)
    (f0, l0), (f1, l1) = bounds(0), bounds(1)
    first_me, last_me = f0 + e * (f1 - f0), l0 + e * (l1 - l0)
    first_it, last_it = f1 + e * (f0 - f1), l1 + e * (l0 - l1)

    def cot_of(s, first, last):
        low = gin[:CAP, s * L : (s + 1) * L].astype(jnp.float32)
        high = gin[CAP:, s * L : (s + 1) * L].astype(jnp.float32)
        source_row = row + jnp.where(row >= first, 0, CAP)
        value = jnp.where(source_row < last, pick(low, high, row, first), 0.0)
        return value.astype(jnp.bfloat16)

    def give(s, src):
        unit = gbuf.at[s, src]
        q = Q_OF[LEFT, s]
        remote(unit, gbuf.at[q, src], gx_s.at[s, 0, src], gx_r.at[q - SUBS, src], right).start()
        q = Q_OF[RIGHT, s]
        remote(unit, gbuf.at[q, src], gx_s.at[s, 1, src], gx_r.at[q - SUBS, src], left).start()

    def to_partner(s):
        gsend[s] = cot_of(s, first_it, last_it)
        remote(gsend.at[s], gbuf.at[s, e], gd_s.at[s], gd_r.at[s], partner).start()

    g_loads[0].wait()
    for load in x_loads:
        load.start()
    gbuf[0, e] = cot_of(0, first_me, last_me)
    pl.semaphore_wait(barrier, 16 - jnp.where(own_dest, 1, 0))
    give(0, e)
    to_partner(0)
    for s in range(1, SUBS):
        g_loads[s].wait()
        to_partner(s)
        gbuf[s, e] = cot_of(s, first_me, last_me)
    for s in range(SUBS):
        wait(gbuf.at[s, 1 - e], gd_r.at[s])
        give(s, 1 - e)
        if s + 1 < SUBS:
            give(s + 1, e)

    def tokens_of(fb, first):
        cols = slice(fb * L, (fb + 1) * L)
        low = xin[:CAP, cols].astype(jnp.float32)
        high = xin[CAP:, cols].astype(jnp.float32)
        return pick(low, high, row, first).astype(jnp.bfloat16).T

    my_rows = pl.ds(pl.multiple_of(e * CAP, CAP), CAP)
    its_rows = pl.ds(pl.multiple_of((1 - e) * CAP, CAP), CAP)
    for fb in range(BLOCKS):
        if fb % 2 == 0:
            x_loads[fb // 2].wait()
        xsend[:, fb] = tokens_of(fb, first_it).reshape(2, L // 2, CAP)
        remote(xsend.at[:, fb], xt.at[:, fb, :, my_rows], xd_s, xd_r, partner).start()
    for fb in range(BLOCKS):
        xt[:, fb, :, my_rows] = tokens_of(fb, first_me).reshape(2, L // 2, CAP)
    wait(xt.at[:, :, :, its_rows], xd_r)

    def receive(q):
        slot, s = ORDER[q]
        if slot != OWN:
            for src in range(2):
                wait(gbuf.at[q, src], gx_r.at[q - SUBS, src])
        o = Q_OF[OPP, s]
        if slot == LEFT:
            remote(gbuf.at[q, 0], gbuf.at[o, 0], gx_s.at[s, 2, 0], gx_r.at[o - SUBS, 0], right).start()
        if slot == RIGHT:
            remote(gbuf.at[q, 1], gbuf.at[o, 1], gx_s.at[s, 2, 1], gx_r.at[o - SUBS, 1], left).start()

    def multiply(group, part):
        grads = jnp.concatenate([gbuf[q].reshape(2 * CAP, L) for q in group], axis=1)
        terms = jnp.dot(
            xt[part].reshape(HALF, 2 * CAP), grads, preferred_element_type=jnp.float32
        )
        for k, q in enumerate(group):
            p[q, :, part] = terms[:, k * L : (k + 1) * L].reshape(BLOCKS, 2, 32, L)

    def view(ref, q, part, *at):
        return ref.at[q, *at, part] if q in SPLIT else ref.at[q, *at]

    def first(q, part=0):
        for m, h, b, to in (
            (3 - y_a, 0, 1, dev_a),
            (4 + y_b + 1 - 2 * (y_b % 2), 1, 1, dev_b),
            (y_a, 0, 0, dev_a),
            (4 + y_b, 1, 0, dev_b),
        ):
            remote(view(p, q, part, m), view(y1, q, part, h, b), y1_s.at[q + part], y1_r.at[q + part], to).start()

    def second(q, part=0):
        wait(view(y1, q, part, slice(None), slice(None)), y1_r.at[q + part])
        for m, h, to in ((y_b, 0, dev_b), (4 + y_a, 1, dev_a)):
            view(p, q, part, m)[...] += view(y1, q, part, h, 1)[...]
            remote(view(p, q, part, m), view(y2, q, part, h), y2_s.at[q + part], y2_r.at[q + part], to).start()
        for m, h in ((y, 0), (4 + y, 1)):
            view(p, q, part, m)[...] += view(y1, q, part, h, 0)[...]

    def piece(q, r):
        return p.at[q, (r // 4) * 4 + y, (r // 2) % 2, r % 2]

    def third(q, part=0):
        wait(view(y2, q, part, slice(None)), y2_r.at[q + part])
        for m, h in ((y, 0), (4 + y, 1)):
            view(p, q, part, m)[...] += view(y2, q, part, h)[...]
        if q not in SPLIT:
            for d in (4, 3, 5, 2, 6, 1, 7):
                zz = (z + d) % 8
                remote(piece(q, rank(zz)), zb.at[q, d - 1], z_s.at[q], z_r.at[q], dev(t, y, zz, e)).start()
            return
        for r in (2 * part, 2 * part + 1, 2 * part + 4, 2 * part + 5):
            zz = (r + 2 * t + 5) % 8

            @pl.when(zz != z)
            def _():
                slot = (zz - z + 7) % 8
                remote(piece(q, r), zb.at[q, slot], z_s.at[q], z_r.at[q], dev(t, y, zz, e)).start()

    def last(q):
        slot, s = ORDER[q]
        wait(zb.at[q], z_r.at[q])
        total = piece(q, my_rank)[...]
        for d in range(7):
            total += zb[q, d]
        fin[q] = total
        to = dev((t + X_OFF[slot]) % 4, y, dest_z, dest_c)
        place = ob.at[e, s, my_rank % 2]
        if slot == OWN:

            @pl.when(own_dest)
            def _():
                pltpu.make_async_copy(fin.at[q], place, f_r).start()

            @pl.when(jnp.logical_not(own_dest))
            def _():
                remote(fin.at[q], place, f_s.at[q], f_r, to).start()
        else:
            remote(fin.at[q], place, f_s.at[q], f_r, to).start()

    stages = {"a": first, "b": second, "c": third, "d": last}
    for entry in PLAN:
        qs = [int(v) for v in entry[1:].split(",")]
        if entry[0] == "m":
            for q in qs:
                receive(q)
            for part in range(2):
                multiply(qs, part)
            if qs[0] in SPLIT:
                first(qs[0], 0)
                first(qs[0], 1)
        elif entry[0].isupper():
            stages[entry[0].lower()](qs[0], 1)
        else:
            stages[entry[0]](qs[0])

    for s in range(SUBS):
        wait(gsend.at[s], gd_s.at[s])
        for way in range(3):
            for src in range(2):
                wait(gbuf.at[s, src], gx_s.at[s, way, src])
    wait(xsend, xd_s)
    for q in range(N_Q):
        for part in range(2 if q in SPLIT else 1):
            wait(view(y1, q, part, slice(None), slice(None)), y1_s.at[q + part])
            wait(view(y2, q, part, slice(None)), y2_s.at[q + part])
        wait(zb.at[q], z_s.at[q])

    wait(ob, f_r)
    for c in range(2):
        for s in range(SUBS):
            for half in range(2):
                out_ref[c, half * 32 : (half + 1) * 32, s * L : (s + 1) * L] = ob[c, s, half]
    for q in range(N_Q):
        if ORDER[q][0] == OWN:

            @pl.when(jnp.logical_not(own_dest))
            def _():
                wait(fin.at[q], f_s.at[q])
        else:
            wait(fin.at[q], f_s.at[q])


def per_device(tokens, cotangent, seg_start, seg_length):
    dma = pltpu.SemaphoreType.DMA
    bf16, f32 = jnp.bfloat16, jnp.float32
    out = pl.pallas_call(
        kernel,
        out_shape=jax.ShapeDtypeStruct((2, 64, SUBS * L), f32),
        in_specs=[pl.BlockSpec(memory_space=pl.ANY)] * 2 + [pl.BlockSpec(memory_space=pltpu.SMEM)] * 2,
        out_specs=pl.BlockSpec(memory_space=pltpu.VMEM),
        scratch_shapes=[
            pltpu.VMEM((2 * CAP, FEATS), bf16),
            pltpu.VMEM((2 * CAP, SUBS * L), bf16),
            pltpu.VMEM((2, BLOCKS, L // 2, 2 * CAP), bf16),
            pltpu.VMEM((2, BLOCKS, L // 2, CAP), bf16),
            pltpu.VMEM((N_Q, 2, CAP, L), bf16),
            pltpu.VMEM((SUBS, CAP, L), bf16),
            pltpu.VMEM((N_Q, BLOCKS, 2, 2, 32, L), f32),
            pltpu.VMEM((N_Q, 2, 2, 2, 2, 32, L), f32),
            pltpu.VMEM((N_Q, 2, 2, 2, 32, L), f32),
            pltpu.VMEM((N_Q, 7, 32, L), f32),
            pltpu.VMEM((N_Q, 32, L), f32),
            pltpu.VMEM((2, SUBS, 2, 32, L), f32),
            dma((SUBS + BLOCKS // 2,)),
            dma((SUBS,)), dma((SUBS,)), dma, dma,
            dma((SUBS, 3, 2)), dma((N_Q - SUBS, 2)),
            dma((N_Q + 1,)), dma((N_Q + 1,)), dma((N_Q + 1,)), dma((N_Q + 1,)), dma((N_Q,)), dma((N_Q,)),
            dma((N_Q,)), dma,
        ],
        compiler_params=pltpu.CompilerParams(
            collective_id=0, has_side_effects=True, vmem_limit_bytes=54000 * 1024
        ),
        cost_estimate=pl.CostEstimate(flops=6442450944, bytes_accessed=6000000, transcendentals=0),
    )(tokens, cotangent, seg_start, seg_length)
    return out.transpose(1, 0, 2)


def solution(mesh):
    in_specs = (P("dp", "tensor"), P("dp", "tensor"), P("dp", None), P("dp", None))
    out_specs = P("dp", None, "tensor")
    return jax.shard_map(
        per_device, mesh=mesh, in_specs=in_specs, out_specs=out_specs, check_vma=False
    )
```

```python
import jax
import jax.numpy as jnp
from jax import lax
from jax.experimental import pallas as pl
from jax.experimental.pallas import tpu as pltpu
from jax.sharding import PartitionSpec as P

MESH = pl.DeviceIdType.MESH
CAP = 1024
FEATS = 1024
L = 128
SUBS = 3
OWN, LEFT, RIGHT, OPP = 0, 1, 2, 3
X_OFF = {OWN: 0, LEFT: 3, RIGHT: 1, OPP: 2}
ORDER = (
    [(OWN, s) for s in range(SUBS)]
    + [(side, s) for s in range(SUBS) for side in (LEFT, RIGHT)]
    + [(OPP, s) for s in range(SUBS)]
)
N_Q = len(ORDER)
Q_OF = {slot_s: q for q, slot_s in enumerate(ORDER)}
BLOCKS = FEATS // L
SPLIT = (N_Q - 1,)
PLAN = (
    "m0,1", "a1", "a0", "m2", "a2", "b1", "b0", "m3,4", "a4", "a3", "b2", "c1", "c0", "b4", "b3", "m5,6",
    "a5", "a6", "c2", "c4", "c3", "b5", "d1", "d0", "b6", "m7,8", "a8", "a7", "c5", "c6", "d2", "d4", "d3",
    "m9", "a9", "b8", "b7", "d5", "m10", "a10", "c8", "c7", "b9", "d6", "m11", "c9", "b10", "d8", "d7", "b11",
    "B11", "c10", "c11", "C11", "d9", "d10", "d11",
)
HALF = FEATS // 2


def kernel(
    tok_hbm, cot_hbm, start_ref, length_ref, out_ref,
    xin, gin, xt, xsend, gbuf, gsend, p, y1, y2, zb, fin, ob,
    in_sem, gd_s, gd_r, xd_s, xd_r, gx_s, gx_r, y1_s, y1_r, y2_s, y2_r, z_s, z_r, f_s, f_r,
):
    t = lax.axis_index("tensor")
    dp = lax.axis_index("dp")
    z, y, e = dp // 8, (dp // 2) % 4, dp % 2

    def dev(x, y, z, c):
        return (z * 8 + y * 2 + c, x)

    def remote(src, dst, s, r, to):
        return pltpu.make_async_remote_copy(
            src_ref=src, dst_ref=dst, send_sem=s, recv_sem=r, device_id=to, device_id_type=MESH
        )

    def wait(ref, sem):
        pltpu.make_async_copy(ref, ref, sem).wait()

    partner = dev(t, y, z, 1 - e)
    right, left = dev((t + 1) % 4, y, z, e), dev((t + 3) % 4, y, z, e)
    y_a, y_b = y + 1 - 2 * (y % 2), 3 - y
    dev_a, dev_b = dev(t, y_a, z, e), dev(t, y_b, z, e)

    def rank(zz):
        return (zz - 2 * t + 11) % 8

    my_rank = rank(z)
    dest_z, dest_c = 2 * t + my_rank // 4, (my_rank // 2) % 2
    own_dest = (dest_z == z) & (dest_c == e)

    g_loads = [
        pltpu.make_async_copy(cot_hbm.at[:, cols], gin.at[:, cols], in_sem.at[s])
        for s, cols in enumerate(pl.ds(s * L, L) for s in range(SUBS))
    ]
    x_loads = [
        pltpu.make_async_copy(tok_hbm.at[:, cols], xin.at[:, cols], in_sem.at[SUBS + i])
        for i, cols in enumerate(pl.ds(i * 2 * L, 2 * L) for i in range(BLOCKS // 2))
    ]
    for load in g_loads:
        load.start()

    barrier = pltpu.get_barrier_semaphore()

    def greet(to):
        pl.semaphore_signal(barrier, inc=1, device_id=to, device_id_type=MESH)

    for to in (partner, right, left, dev_a, dev_b):
        greet(to)
    for d in range(1, 8):
        greet(dev(t, y, (z + d) % 8, e))
    for half in range(2):
        for c in range(2):
            sx = z // 2
            sz = (4 * (z % 2) + 2 * e + half + 2 * sx + 5) % 8

            @pl.when(jnp.logical_not((sx == t) & (sz == z) & (c == e)))
            def _():
                greet(dev(sx, y, sz, c))

    def bounds(expert):
        first = start_ref[0, expert]
        return first, first + length_ref[0, expert]

    def pick(low, high, row, first):
        return jnp.where(row >= first, low, high)

    row = lax.broadcasted_iota(jnp.int32, (CAP, L), 0)
    (f0, l0), (f1, l1) = bounds(0), bounds(1)
    first_me, last_me = f0 + e * (f1 - f0), l0 + e * (l1 - l0)
    first_it, last_it = f1 + e * (f0 - f1), l1 + e * (l0 - l1)

    def cot_of(s, first, last):
        low = gin[:CAP, s * L : (s + 1) * L].astype(jnp.float32)
        high = gin[CAP:, s * L : (s + 1) * L].astype(jnp.float32)
        source_row = row + jnp.where(row >= first, 0, CAP)
        value = jnp.where(source_row < last, pick(low, high, row, first), 0.0)
        return value.astype(jnp.bfloat16)

    def give(s, src):
        unit = gbuf.at[s, src]
        q = Q_OF[LEFT, s]
        remote(unit, gbuf.at[q, src], gx_s.at[s, 0, src], gx_r.at[q - SUBS, src], right).start()
        q = Q_OF[RIGHT, s]
        remote(unit, gbuf.at[q, src], gx_s.at[s, 1, src], gx_r.at[q - SUBS, src], left).start()

    def to_partner(s):
        gsend[s] = cot_of(s, first_it, last_it)
        remote(gsend.at[s], gbuf.at[s, e], gd_s.at[s], gd_r.at[s], partner).start()

    g_loads[0].wait()
    for load in x_loads:
        load.start()
    gbuf[0, e] = cot_of(0, first_me, last_me)
    pl.semaphore_wait(barrier, 16 - jnp.where(own_dest, 1, 0))
    give(0, e)
    to_partner(0)
    for s in range(1, SUBS):
        g_loads[s].wait()
        to_partner(s)
        gbuf[s, e] = cot_of(s, first_me, last_me)
    for s in range(SUBS):
        wait(gbuf.at[s, 1 - e], gd_r.at[s])
        give(s, 1 - e)
        if s + 1 < SUBS:
            give(s + 1, e)

    def tokens_of(fb, first):
        cols = slice(fb * L, (fb + 1) * L)
        low = xin[:CAP, cols].astype(jnp.float32)
        high = xin[CAP:, cols].astype(jnp.float32)
        return pick(low, high, row, first).astype(jnp.bfloat16).T

    my_rows = pl.ds(pl.multiple_of(e * CAP, CAP), CAP)
    its_rows = pl.ds(pl.multiple_of((1 - e) * CAP, CAP), CAP)
    for fb in range(BLOCKS):
        if fb % 2 == 0:
            x_loads[fb // 2].wait()
        xsend[:, fb] = tokens_of(fb, first_it).reshape(2, L // 2, CAP)
        remote(xsend.at[:, fb], xt.at[:, fb, :, my_rows], xd_s, xd_r, partner).start()
    for fb in range(BLOCKS):
        xt[:, fb, :, my_rows] = tokens_of(fb, first_me).reshape(2, L // 2, CAP)
    wait(xt.at[:, :, :, its_rows], xd_r)

    def receive(q):
        slot, s = ORDER[q]
        if slot != OWN:
            for src in range(2):
                wait(gbuf.at[q, src], gx_r.at[q - SUBS, src])
        o = Q_OF[OPP, s]
        if slot == LEFT:
            remote(gbuf.at[q, 0], gbuf.at[o, 0], gx_s.at[s, 2, 0], gx_r.at[o - SUBS, 0], right).start()
        if slot == RIGHT:
            remote(gbuf.at[q, 1], gbuf.at[o, 1], gx_s.at[s, 2, 1], gx_r.at[o - SUBS, 1], left).start()

    def multiply(group, part):
        grads = jnp.concatenate([gbuf[q].reshape(2 * CAP, L) for q in group], axis=1)
        terms = jnp.dot(
            xt[part].reshape(HALF, 2 * CAP), grads, preferred_element_type=jnp.float32
        )
        for k, q in enumerate(group):
            p[q, :, part] = terms[:, k * L : (k + 1) * L].reshape(BLOCKS, 2, 32, L)

    def view(ref, q, part, *at):
        return ref.at[q, *at, part] if q in SPLIT else ref.at[q, *at]

    def first(q, part=0):
        for m, h, b, to in (
            (3 - y_a, 0, 1, dev_a),
            (4 + y_b + 1 - 2 * (y_b % 2), 1, 1, dev_b),
            (y_a, 0, 0, dev_a),
            (4 + y_b, 1, 0, dev_b),
        ):
            remote(view(p, q, part, m), view(y1, q, part, h, b), y1_s.at[q + part], y1_r.at[q + part], to).start()

    def second(q, part=0):
        wait(view(y1, q, part, slice(None), slice(None)), y1_r.at[q + part])
        for m, h, to in ((y_b, 0, dev_b), (4 + y_a, 1, dev_a)):
            view(p, q, part, m)[...] += view(y1, q, part, h, 1)[...]
            remote(view(p, q, part, m), view(y2, q, part, h), y2_s.at[q + part], y2_r.at[q + part], to).start()
        for m, h in ((y, 0), (4 + y, 1)):
            view(p, q, part, m)[...] += view(y1, q, part, h, 0)[...]

    def piece(q, r):
        return p.at[q, (r // 4) * 4 + y, (r // 2) % 2, r % 2]

    def third(q, part=0):
        wait(view(y2, q, part, slice(None)), y2_r.at[q + part])
        for m, h in ((y, 0), (4 + y, 1)):
            view(p, q, part, m)[...] += view(y2, q, part, h)[...]
        if q not in SPLIT:
            for d in (4, 3, 5, 2, 6, 1, 7):
                zz = (z + d) % 8
                remote(piece(q, rank(zz)), zb.at[q, d - 1], z_s.at[q], z_r.at[q], dev(t, y, zz, e)).start()
            return
        for r in (2 * part, 2 * part + 1, 2 * part + 4, 2 * part + 5):
            zz = (r + 2 * t + 5) % 8

            @pl.when(zz != z)
            def _():
                slot = (zz - z + 7) % 8
                remote(piece(q, r), zb.at[q, slot], z_s.at[q], z_r.at[q], dev(t, y, zz, e)).start()

    def last(q):
        slot, s = ORDER[q]
        wait(zb.at[q], z_r.at[q])
        total = piece(q, my_rank)[...]
        for d in range(7):
            total += zb[q, d]
        fin[q] = total
        to = dev((t + X_OFF[slot]) % 4, y, dest_z, dest_c)
        place = ob.at[e, s, my_rank % 2]
        if slot == OWN:

            @pl.when(own_dest)
            def _():
                pltpu.make_async_copy(fin.at[q], place, f_r).start()

            @pl.when(jnp.logical_not(own_dest))
            def _():
                remote(fin.at[q], place, f_s.at[q], f_r, to).start()
        else:
            remote(fin.at[q], place, f_s.at[q], f_r, to).start()

    stages = {"a": first, "b": second, "c": third, "d": last}
    for entry in PLAN:
        qs = [int(v) for v in entry[1:].split(",")]
        if entry[0] == "m":
            for q in qs:
                receive(q)
            for part in range(2):
                multiply(qs, part)
            if qs[0] in SPLIT:
                first(qs[0], 0)
                first(qs[0], 1)
        elif entry[0].isupper():
            stages[entry[0].lower()](qs[0], 1)
        else:
            stages[entry[0]](qs[0])

    for s in range(SUBS):
        wait(gsend.at[s], gd_s.at[s])
        for way in range(3):
            for src in range(2):
                wait(gbuf.at[s, src], gx_s.at[s, way, src])
    wait(xsend, xd_s)
    for q in range(N_Q):
        for part in range(2 if q in SPLIT else 1):
            wait(view(y1, q, part, slice(None), slice(None)), y1_s.at[q + part])
            wait(view(y2, q, part, slice(None)), y2_s.at[q + part])
        wait(zb.at[q], z_s.at[q])

    wait(ob, f_r)
    for c in range(2):
        for s in range(SUBS):
            for half in range(2):
                out_ref[c, half * 32 : (half + 1) * 32, s * L : (s + 1) * L] = ob[c, s, half]
    for q in range(N_Q):
        if ORDER[q][0] == OWN:

            @pl.when(jnp.logical_not(own_dest))
            def _():
                wait(fin.at[q], f_s.at[q])
        else:
            wait(fin.at[q], f_s.at[q])


def per_device(tokens, cotangent, seg_start, seg_length):
    dma = pltpu.SemaphoreType.DMA
    bf16, f32 = jnp.bfloat16, jnp.float32
    out = pl.pallas_call(
        kernel,
        out_shape=jax.ShapeDtypeStruct((2, 64, SUBS * L), f32),
        in_specs=[pl.BlockSpec(memory_space=pl.ANY)] * 2 + [pl.BlockSpec(memory_space=pltpu.SMEM)] * 2,
        out_specs=pl.BlockSpec(memory_space=pltpu.VMEM),
        scratch_shapes=[
            pltpu.VMEM((2 * CAP, FEATS), bf16),
            pltpu.VMEM((2 * CAP, SUBS * L), bf16),
            pltpu.VMEM((2, BLOCKS, L // 2, 2 * CAP), bf16),
            pltpu.VMEM((2, BLOCKS, L // 2, CAP), bf16),
            pltpu.VMEM((N_Q, 2, CAP, L), bf16),
            pltpu.VMEM((SUBS, CAP, L), bf16),
            pltpu.VMEM((N_Q, BLOCKS, 2, 2, 32, L), f32),
            pltpu.VMEM((N_Q, 2, 2, 2, 2, 32, L), f32),
            pltpu.VMEM((N_Q, 2, 2, 2, 32, L), f32),
            pltpu.VMEM((N_Q, 7, 32, L), f32),
            pltpu.VMEM((N_Q, 32, L), f32),
            pltpu.VMEM((2, SUBS, 2, 32, L), f32),
            dma((SUBS + BLOCKS // 2,)),
            dma((SUBS,)), dma((SUBS,)), dma, dma,
            dma((SUBS, 3, 2)), dma((N_Q - SUBS, 2)),
            dma((N_Q + 1,)), dma((N_Q + 1,)), dma((N_Q + 1,)), dma((N_Q + 1,)), dma((N_Q,)), dma((N_Q,)),
            dma((N_Q,)), dma,
        ],
        compiler_params=pltpu.CompilerParams(
            collective_id=0, has_side_effects=True, vmem_limit_bytes=54000 * 1024
        ),
        cost_estimate=pl.CostEstimate(flops=6442450944, bytes_accessed=6000000, transcendentals=0),
    )(tokens, cotangent, seg_start, seg_length)
    return out.transpose(1, 0, 2)


def solution(mesh):
    in_specs = (P("dp", "tensor"), P("dp", "tensor"), P("dp", None), P("dp", None))
    out_specs = P("dp", None, "tensor")
    return jax.shard_map(
        per_device, mesh=mesh, in_specs=in_specs, out_specs=out_specs, check_vma=False
    )
```
